32 devices in a mesh: mod: 2 (over y), dp: 16 (over z, x, core).
Axes of the slice: x: 2, y: 2, z: 4, core: 2. Of those that a mesh axis runs over, the one named last changes fastest.
Arguments:
- image_pooled: bfloat16 [640, 1024], P('dp'), may hold values from -6 to 6
- text_pooled: bfloat16 [640, 768], P('dp'), may hold values from -6 to 6
- image_gain: float32 [1024], replicated, may hold values from 0.25 to 1.75
- text_gain: float32 [768], replicated, may hold values from 0.25 to 1.75
- image_proj: bfloat16 [1024, 768], replicated, may hold values from -0.1875 to 0.1875
- text_proj: bfloat16 [768, 768], replicated, may hold values from -0.21875 to 0.21875
- logit_scale: float32 [1], replicated, may hold values from 10 to 100
- pair_index: int32 [2, 640], P('mod', 'dp'), may hold values from 0 to 639, as said below
Outputs:
- loss_value: float32 [], replicated
- embed_grad: float32 [2, 640, 768], P('mod', 'dp')
The draws below stay inside these ranges and needn't reach their ends.
Inputs may be any that keep to these rules, and one draw needn't show every extreme that they name: `pair_index`: row 0 is a permutation of 0 to 639 and row 1 is its inverse permutation.
All inputs are finite; a program needn't handle non-finite values.
Results may differ from the reference program's by a relative error of at most 0.0041.
Values may be sent and summed in bfloat16 or wider, within the bound.
A program may use at most 128 MiB of HBM per device.

```python
import math
import jax
import jax.numpy as jnp
from jax import lax

DI = 1024
DT = 768
EMBED = 768
ROWS = 40
BATCH = 640
N_DP = 16


def draw_pair_index(key, part):
    forward = jax.random.permutation(jax.random.fold_in(key, 11), BATCH).astype(jnp.int32)
    inverse = jnp.argsort(forward, stable=True).astype(jnp.int32)
    return jnp.stack([forward, inverse])


def shard_levels(rng, extent, pieces, smallest, largest):
    def one(dim, blocks):
        heights = jax.random.uniform(jax.random.fold_in(jax.random.fold_in(rng, 6), dim), (blocks,), jnp.float32, smallest / len(pieces), largest / len(pieces))
        return jnp.repeat(jnp.exp(heights), extent[dim] // blocks).reshape((-1,) + (1,) * (len(extent) - dim - 1))

    level = one(*pieces[0])
    for cut in pieces[1:]:
        level = level * one(*cut)
    return level


def noise(key, shape, spread, limit, split=(), held_as=jnp.bfloat16):
    entries = spread * jax.random.normal(key, shape, jnp.float32)
    if split:
        entries = entries * shard_levels(key, shape, split, -0.22, 0.18)
    return jnp.clip(entries, -limit, limit).astype(held_as)


def setup_inputs(seed: int = 0) -> dict:
    streams_of = jax.random.split(jax.random.key(seed), 9)
    return {
        "image_pooled": noise(streams_of[0], (BATCH, DI), 1.0, 6.0, ((0, 16),)),
        "text_pooled": noise(streams_of[1], (BATCH, DT), 1.0, 6.0, ((0, 16),)),
        "image_gain": jnp.clip(1.0 + 0.15 * jax.random.normal(streams_of[2], (DI,), jnp.float32), 0.25, 1.75),
        "text_gain": jnp.clip(1.0 + 0.15 * jax.random.normal(streams_of[3], (DT,), jnp.float32), 0.25, 1.75),
        "image_proj": noise(streams_of[4], (DI, EMBED), DI ** -0.5, 0.1875),
        "text_proj": noise(streams_of[5], (DT, EMBED), DT ** -0.5, 0.21875),
        "logit_scale": jnp.clip(jnp.exp(jax.random.uniform(streams_of[6], (1,), jnp.float32, math.log(10.0), math.log(100.0))), 10.0, 100.0),
        "pair_index": draw_pair_index(jax.random.fold_in(streams_of[8], 71), 0),
    }


def normalize_project(pooled, gain, weight):
    features = pooled.astype(jnp.float32)
    centered = features - lax.optimization_barrier(jnp.mean(features, axis=-1, keepdims=True))
    variance = lax.optimization_barrier(jnp.mean(centered * centered, axis=-1, keepdims=True))
    normalized = (centered * lax.rsqrt(variance + 1e-05) * gain).astype(jnp.bfloat16)
    return jnp.dot(normalized, weight, preferred_element_type=jnp.float32)

def unitize(embedded):
    lengths = jnp.sqrt(lax.optimization_barrier(jnp.sum(embedded * embedded, axis=-1, keepdims=True)) + 1e-06)
    return (embedded / lengths, lengths)

def similarity(left_rows, right_rows, scale_value):
    return scale_value * lax.dot_general(left_rows, right_rows, (((1,), (1,)), ((), ())), preferred_element_type=jnp.float32)

def lse_pass(own_half, other_half, partners, scale_value):
    width = own_half.shape[1]

    def one_block(inputs):
        block_rows, block_pairs = inputs
        score_block = similarity(block_rows, other_half, scale_value)
        running_max = lax.optimization_barrier(jnp.max(score_block, axis=1))
        block_lse = running_max + jnp.log(lax.optimization_barrier(jnp.sum(jnp.exp(score_block - running_max[:, None]), axis=1)))
        columns = lax.broadcasted_iota(jnp.int32, score_block.shape, 1)
        matched = columns == block_pairs[:, None]
        block_diag = lax.optimization_barrier(jnp.sum(jnp.where(matched, score_block, 0.0), axis=1))
        return (block_lse, block_diag)
    lse_blocks, diag_blocks = lax.map(one_block, (own_half.reshape(N_DP, ROWS, width), partners.reshape(N_DP, ROWS)))
    return (lse_blocks.reshape(-1), diag_blocks.reshape(-1))

def grad_pass(own_half, other_half, own_lse, other_lse, partners, scale_value, unit_rows, lengths):
    width = own_half.shape[1]
    batch_total = own_half.shape[0]

    def one_block(inputs):
        block_rows, block_lse, block_pairs, block_unit, block_len = inputs
        score_block = similarity(block_rows, other_half, scale_value)
        columns = lax.broadcasted_iota(jnp.int32, score_block.shape, 1)
        matched = (columns == block_pairs[:, None]).astype(jnp.float32)
        pair_weight = (jnp.exp(score_block - block_lse[:, None]) + jnp.exp(score_block - other_lse[None, :]) - 2.0 * matched).astype(jnp.bfloat16)
        unit_grad = scale_value / (2.0 * batch_total) * jnp.dot(pair_weight, other_half, preferred_element_type=jnp.float32)
        return (unit_grad - block_unit * lax.optimization_barrier(jnp.sum(block_unit * unit_grad, axis=-1, keepdims=True))) / block_len
    grad_blocks = lax.map(one_block, (own_half.reshape(N_DP, ROWS, width), own_lse.reshape(N_DP, ROWS), partners.reshape(N_DP, ROWS), unit_rows.reshape(N_DP, ROWS, width), lengths.reshape(N_DP, ROWS, 1)))
    return grad_blocks.reshape(batch_total, width)

def reference(image_pooled, text_pooled, image_gain, text_gain, image_proj, text_proj, logit_scale, pair_index):
    image_unit, image_len = unitize(normalize_project(image_pooled, image_gain, image_proj))
    text_unit, text_len = unitize(normalize_project(text_pooled, text_gain, text_proj))
    image_half = image_unit.astype(jnp.bfloat16)
    text_half = text_unit.astype(jnp.bfloat16)
    scale_value = logit_scale[0]
    image_lse, image_diag = lse_pass(image_half, text_half, pair_index[0], scale_value)
    text_lse, text_diag = lse_pass(text_half, image_half, pair_index[1], scale_value)
    batch_total = image_half.shape[0]
    loss_value = (jnp.sum(image_lse - image_diag) + jnp.sum(text_lse - text_diag)) / (2.0 * batch_total)
    image_grad = grad_pass(image_half, text_half, image_lse, text_lse, pair_index[0], scale_value, image_unit, image_len)
    text_grad = grad_pass(text_half, image_half, text_lse, image_lse, pair_index[1], scale_value, text_unit, text_len)
    return (loss_value, jnp.stack([image_grad, text_grad]))
```

```python
import functools

import jax
import jax.numpy as jnp
from jax import lax
from jax.experimental import pallas as pl
from jax.experimental.pallas import tpu as pltpu
from jax.sharding import PartitionSpec as P

MESH = pl.DeviceIdType.MESH
UNROLL = 32


def loop(count, body):
    if count <= UNROLL:
        for step in range(count):
            body(step)
    else:
        pl.loop(0, count)(body)


def fold(count, body, init):
    if count <= UNROLL:
        for step in range(count):
            init = body(step, init)
        return init
    return lax.fori_loop(0, count, body, init)


def kernel(
    n_mod, n_dp,
    image_ref, text_ref, image_gain_ref, text_gain_ref, image_proj_ref, text_proj_ref, scale_ref, pair_ref,
    loss_ref, grad_ref,
    image_w, text_w, rows_all, unit, length, scores, base, note, notes,
    w_sem, send_sem, recv_sem, note_send, note_recv,
):
    module, me = lax.axis_index("mod"), lax.axis_index("dp")
    n_all = n_mod * n_dp
    n_line = n_dp // 4
    line, side, core = me // 4, (me // 2) % 2, me % 2
    here = module * n_dp + me
    row_count = image_ref.shape[0]
    across = (line * 2 + (1 - side)) * 2 + core
    twin = me + 1 - 2 * core

    image_copy = pltpu.make_async_copy(image_proj_ref, image_w, w_sem.at[0])
    text_copy = pltpu.make_async_copy(text_proj_ref, text_w, w_sem.at[1])

    @pl.when(module == 0)
    def _():
        text_copy.start()
        image_copy.start()

    @pl.when(module != 0)
    def _():
        image_copy.start()
        text_copy.start()

    barrier = pltpu.get_barrier_semaphore()

    def greet(step):
        other = (here + step + 1) % n_all
        pl.semaphore_signal(
            barrier, inc=1, device_id=(other // n_dp, other % n_dp), device_id_type=MESH
        )

    loop(n_all - 1, greet)

    def embed(pooled_ref, gain_ref, copy, w):
        features = pooled_ref[...].astype(jnp.float32)
        centered = features - jnp.mean(features, axis=-1, keepdims=True)
        variance = jnp.mean(centered * centered, axis=-1, keepdims=True)
        normed = centered * lax.rsqrt(variance + 1e-05) * gain_ref[...].reshape(1, -1)
        normed = normed.astype(jnp.bfloat16)
        copy.wait()
        embedded = jnp.dot(normed, w[...], preferred_element_type=jnp.float32)
        lengths = jnp.sqrt(jnp.sum(embedded * embedded, axis=-1, keepdims=True) + 1e-06)
        return embedded / lengths, lengths

    def embed_other(*args):
        rows, _ = embed(*args)
        rows_all[me] = rows.astype(jnp.bfloat16)

    def embed_own(*args):
        unit[...], length[...] = embed(*args)

    image_args = (image_ref, image_gain_ref, image_copy, image_w)
    text_args = (text_ref, text_gain_ref, text_copy, text_w)

    pl.when(module == 0)(lambda: embed_other(*text_args))
    pl.when(module != 0)(lambda: embed_other(*image_args))

    pl.semaphore_wait(barrier, n_all - 1)

    def send(block, target, sem):
        return pltpu.make_async_remote_copy(
            src_ref=rows_all.at[block], dst_ref=rows_all.at[block],
            send_sem=send_sem.at[sem], recv_sem=recv_sem.at[block],
            device_id=(module, target), device_id_type=MESH,
        )

    def on_line(step):
        return (line + step) % n_line

    def peer(step, b, c):
        return (on_line(step) * 2 + b) * 2 + c

    def line_send(step):
        return send(me, peer(step, side, core), step)

    def across_send(step):
        return send(peer(step, side, core), across, n_line + step)

    def twin_send(step, b):
        return send(peer(step, b, core), twin, n_line * (2 + (b + side) % 2) + step)

    across_send(0).start()
    loop(n_line - 1, lambda step: line_send(step + 1).start())
    twin_send(0, side).start()

    pl.when(module == 0)(lambda: embed_own(*image_args))
    pl.when(module != 0)(lambda: embed_own(*text_args))
    own_half = unit[...].astype(jnp.bfloat16)
    scale_value = scale_ref[0]

    def score(block):
        scores[block] = scale_value * lax.dot_general(
            own_half, rows_all[block], (((1,), (1,)), ((), ())), preferred_element_type=jnp.float32
        )

    def arrive(block):
        send(block, twin, 0).wait_recv()

    score(me)

    def from_line(step):
        block = peer(step + 1, side, core)
        arrive(block)
        across_send(step + 1).start()
        twin_send(step + 1, side).start()
        score(block)

    def from_across(step):
        block = peer(step, 1 - side, core)
        arrive(block)
        twin_send(step, 1 - side).start()
        score(block)

    def from_twin(b, step):
        block = peer(step, b, 1 - core)
        arrive(block)
        score(block)

    loop(n_line - 1, from_line)
    loop(n_line, from_across)
    loop(n_line, functools.partial(from_twin, side))
    loop(n_line, functools.partial(from_twin, 1 - side))

    square = (row_count, row_count)
    down = lax.broadcasted_iota(jnp.int32, square, 0)
    over = lax.broadcasted_iota(jnp.int32, square, 1)
    pairs = jnp.sum(
        jnp.where(down == over, pair_ref[...].astype(jnp.float32), 0.0), axis=1, keepdims=True
    ).astype(jnp.int32)

    def matched(block):
        return over + block * row_count == pairs

    peak = fold(n_dp, lambda p, acc: jnp.maximum(acc, scores[p]), jnp.full(square, -jnp.inf, jnp.float32))
    peak = jnp.max(peak, axis=1, keepdims=True)

    def gather_sums(p, acc):
        total, diagonal = acc
        block = scores[p]
        return total + jnp.exp(block - peak), diagonal + jnp.where(matched(p), block, 0.0)

    zero = jnp.zeros(square, jnp.float32)
    total, diagonal = fold(n_dp, gather_sums, (zero, zero))
    lse = peak + jnp.log(jnp.sum(total, axis=1, keepdims=True))
    excess = lse - jnp.sum(diagonal, axis=1, keepdims=True)

    lanes = note.shape[-1]
    wide = (row_count, lanes)
    lane = lax.broadcasted_iota(jnp.int32, wide, 1)
    placed = jnp.where(
        lane == lax.broadcasted_iota(jnp.int32, wide, 0), lse, jnp.where(lane == lanes - 1, excess, 0.0)
    )
    note[...] = jnp.sum(placed, axis=0, keepdims=True)
    notes[here] = note[...]

    def note_copy(step):
        other = (here + step + 1) % n_all
        return pltpu.make_async_remote_copy(
            src_ref=note, dst_ref=notes.at[here],
            send_sem=note_send.at[step], recv_sem=note_recv.at[here],
            device_id=(other // n_dp, other % n_dp), device_id_type=MESH,
        )

    loop(n_all - 1, lambda step: note_copy(step).start())

    def first_half(p):
        base[p] = jnp.exp(scores[p] - lse) - jnp.where(matched(p), 2.0, 0.0)

    loop(n_dp, first_half)

    def note_arrive(step):
        other = (here + step + 1) % n_all
        pltpu.make_async_remote_copy(
            src_ref=note, dst_ref=notes.at[other],
            send_sem=note_send.at[step], recv_sem=note_recv.at[other],
            device_id=(other // n_dp, other % n_dp), device_id_type=MESH,
        ).wait_recv()

    loop(n_all - 1, note_arrive)

    loss = fold(n_all, lambda p, acc: acc + notes[p], jnp.zeros((1, lanes), jnp.float32))
    loss_ref[...] = loss[:, lanes - 1 :] / (2.0 * n_dp * row_count)

    def weigh(p, acc):
        other = notes[(1 - module) * n_dp + p][:, :row_count]
        weight = (base[p] + jnp.exp(scores[p] - other)).astype(jnp.bfloat16)
        return acc + jnp.dot(weight, rows_all[p], preferred_element_type=jnp.float32)

    moved = fold(n_dp, weigh, jnp.zeros(grad_ref.shape[1:], jnp.float32))
    moved = scale_value / (2.0 * n_dp * row_count) * moved
    own = unit[...]
    grad_ref[0] = (moved - own * jnp.sum(own * moved, axis=-1, keepdims=True)) / length[...]

    loop(n_line - 1, lambda step: line_send(step + 1).wait_send())
    loop(n_line, lambda step: across_send(step).wait_send())
    loop(n_line, lambda step: twin_send(step, side).wait_send())
    loop(n_line, lambda step: twin_send(step, 1 - side).wait_send())
    loop(n_all - 1, lambda step: note_copy(step).wait_send())


def solution(mesh):
    n_mod, n_dp = mesh.shape["mod"], mesh.shape["dp"]

    def local(
        image_pooled, text_pooled, image_gain, text_gain, image_proj, text_proj, logit_scale, pair_index
    ):
        rows = image_pooled.shape[0]
        width = image_proj.shape[1]
        lanes = -(-(rows + 1) // 128) * 128
        n_all = n_mod * n_dp
        vmem = pl.BlockSpec(memory_space=pltpu.VMEM)
        anywhere = pl.BlockSpec(memory_space=pl.ANY)
        dma = pltpu.SemaphoreType.DMA
        loss, grad = pl.pallas_call(
            functools.partial(kernel, n_mod, n_dp),
            out_shape=(
                jax.ShapeDtypeStruct((1, 1), jnp.float32),
                jax.ShapeDtypeStruct((1, rows, width), jnp.float32),
            ),
            in_specs=[vmem] * 4 + [anywhere] * 2 + [pl.BlockSpec(memory_space=pltpu.SMEM), vmem],
            out_specs=(vmem, vmem),
            scratch_shapes=[
                pltpu.VMEM(image_proj.shape, image_proj.dtype),
                pltpu.VMEM(text_proj.shape, text_proj.dtype),
                pltpu.VMEM((n_dp, rows, width), jnp.bfloat16),
                pltpu.VMEM((rows, width), jnp.float32),
                pltpu.VMEM((rows, 1), jnp.float32),
                pltpu.VMEM((n_dp, rows, rows), jnp.float32),
                pltpu.VMEM((n_dp, rows, rows), jnp.float32),
                pltpu.VMEM((1, lanes), jnp.float32),
                pltpu.VMEM((n_all, 1, lanes), jnp.float32),
                dma((2,)),
                dma((n_dp,)),
                dma((n_dp,)),
                dma((n_all,)),
                dma((n_all,)),
            ],
            compiler_params=pltpu.CompilerParams(collective_id=0, has_side_effects=True),
        )(image_pooled, text_pooled, image_gain, text_gain, image_proj, text_proj, logit_scale, pair_index)
        return loss[0, 0], grad

    in_specs = (P("dp", None), P("dp", None), P(), P(), P(), P(), P(), P("mod", "dp"))
    out_specs = (P(), P("mod", "dp", None))
    return jax.shard_map(local, mesh=mesh, in_specs=in_specs, out_specs=out_specs, check_vma=False)
```

```python
import functools

import jax
import jax.numpy as jnp
from jax import lax
from jax.experimental import pallas as pl
from jax.experimental.pallas import tpu as pltpu
from jax.sharding import PartitionSpec as P

MESH = pl.DeviceIdType.MESH
UNROLL = 32
CHUNKS = 2


def pick(index, values):
    chosen = 0
    for at, value in enumerate(values):
        chosen = chosen + jnp.where(index == at, value, 0)
    return chosen


def by_distance(index, count, step, far):
    if count > 8:
        return (index + 1 + step) % count
    tables = [
        sorted((p for p in range(count) if p != i), key=lambda p: -abs(p - i) if far else abs(p - i))[step]
        for i in range(count)
    ]
    return pick(index, tables)


def loop(count, body):
    if count <= UNROLL:
        for step in range(count):
            body(step)
    else:
        pl.loop(0, count)(body)


def fold(count, body, init):
    if count <= UNROLL:
        for step in range(count):
            init = body(step, init)
        return init
    return lax.fori_loop(0, count, body, init)


def kernel(
    n_mod, n_dp,
    image_hbm, text_hbm, image_gain_hbm, text_gain_hbm, image_proj_ref, text_proj_ref, scale_hbm, pair_hbm,
    loss_ref, grad_ref,
    image_ref, text_ref, image_gain_ref, text_gain_ref, scale_ref, pair_ref,
    image_w, text_w, rows_all, unit, length, scores, base, note, notes,
    in_sem, w_sem, send_sem, recv_sem, note_send, note_recv, ready,
):
    module, me = lax.axis_index("mod"), lax.axis_index("dp")
    n_all = n_mod * n_dp
    n_line = n_dp // 4
    line, side, core = me // 4, (me // 2) % 2, me % 2
    here = module * n_dp + me
    row_count = image_ref.shape[0]
    across = (line * 2 + (1 - side)) * 2 + core
    twin = me + 1 - 2 * core
    mirror = 1 - module

    def peer(q, b, c):
        return (q * 2 + b) * 2 + c

    barrier = pltpu.get_barrier_semaphore()

    def greet(target_module, target):
        pl.semaphore_signal(barrier, inc=1, device_id=(target_module, target), device_id_type=MESH)

    loop(n_line - 1, lambda step: greet(module, peer((line + step + 1) % n_line, side, core)))
    greet(module, across)
    greet(module, twin)
    greet(mirror, me)

    image_copy = pltpu.make_async_copy(image_proj_ref, image_w, w_sem.at[0])
    text_copy = pltpu.make_async_copy(text_proj_ref, text_w, w_sem.at[1])
    small = [
        pltpu.make_async_copy(source, target, in_sem.at[at])
        for at, (source, target) in enumerate([
            (image_hbm, image_ref), (text_hbm, text_ref), (image_gain_hbm, image_gain_ref),
            (text_gain_hbm, text_gain_ref), (scale_hbm, scale_ref), (pair_hbm, pair_ref),
        ])
    ]
    for copy in small[:4]:
        copy.start()

    @pl.when(module == 0)
    def _():
        text_copy.start()
        image_copy.start()

    @pl.when(module != 0)
    def _():
        image_copy.start()
        text_copy.start()

    for copy in small[4:]:
        copy.start()
    for copy in small:
        copy.wait()

    def embed(pooled_ref, gain_ref, copy, w):
        features = pooled_ref[...].astype(jnp.float32)
        centered = features - jnp.mean(features, axis=-1, keepdims=True)
        variance = jnp.mean(centered * centered, axis=-1, keepdims=True)
        normed = centered * lax.rsqrt(variance + 1e-05) * gain_ref[...].reshape(1, -1)
        normed = normed.astype(jnp.bfloat16)
        copy.wait()
        embedded = jnp.dot(normed, w[...], preferred_element_type=jnp.float32)
        lengths = jnp.sqrt(jnp.sum(embedded * embedded, axis=-1, keepdims=True) + 1e-06)
        return embedded / lengths, lengths

    depth = rows_all.shape[-1]

    def embed_other(*args):
        rows = embed(*args)[0].astype(jnp.bfloat16)
        for h in range(CHUNKS):
            rows_all[me, h] = rows[:, h * depth : (h + 1) * depth]

    def embed_own(*args):
        unit[...], length[...] = embed(*args)

    image_args = (image_ref, image_gain_ref, image_copy, image_w)
    text_args = (text_ref, text_gain_ref, text_copy, text_w)

    pl.when(module == 0)(lambda: embed_other(*text_args))
    pl.when(module != 0)(lambda: embed_other(*image_args))

    pl.semaphore_wait(barrier, n_line + 2)

    def send(block, h, target, sem):
        return pltpu.make_async_remote_copy(
            src_ref=rows_all.at[block, h], dst_ref=rows_all.at[block, h],
            send_sem=send_sem.at[sem, h], recv_sem=recv_sem.at[block, h],
            device_id=(module, target), device_id_type=MESH,
        )

    def line_send(step, h):
        return send(me, h, peer(by_distance(line, n_line, step, True), side, core), step)

    def across_send(q, h, step):
        return send(peer(q, side, core), h, across, n_line + step)

    def twin_send(q, b, h, step):
        return send(peer(q, b, core), h, twin, n_line * 2 + step)

    for h in range(CHUNKS):
        across_send(line, h, 0).start()
        loop(n_line - 1, lambda step: line_send(step, h).start())
        twin_send(line, side, h, 0).start()

    pl.when(module == 0)(lambda: embed_own(*image_args))
    pl.when(module != 0)(lambda: embed_own(*text_args))
    own_half = unit[...].astype(jnp.bfloat16)
    scale_value = scale_ref[0]

    def score(block):
        products = 0.0
        for h in range(CHUNKS):
            products = products + lax.dot_general(
                own_half[:, h * depth : (h + 1) * depth], rows_all[block, h],
                (((1,), (1,)), ((), ())), preferred_element_type=jnp.float32,
            )
        scores[block] = scale_value * products

    def arrive(block, h):
        send(block, h, twin, 0).wait_recv()

    score(me)

    for h in range(CHUNKS):
        arrive(across, h)
        twin_send(line, 1 - side, h, n_line).start()
    score(across)

    def from_line(step):
        q = by_distance(line, n_line, step, False)
        for h in range(CHUNKS):
            arrive(peer(q, side, core), h)
            across_send(q, h, step + 1).start()
            twin_send(q, side, h, step + 1).start()
        score(peer(q, side, core))

    def from_across(step):
        q = by_distance(line, n_line, step, False)
        for h in range(CHUNKS):
            arrive(peer(q, 1 - side, core), h)
            twin_send(q, 1 - side, h, n_line + step + 1).start()
        score(peer(q, 1 - side, core))

    def from_twin(b, q):
        block = peer(q, b, 1 - core)
        for h in range(CHUNKS):
            arrive(block, h)
        score(block)

    from_twin(side, line)
    from_twin(1 - side, line)
    loop(n_line - 1, from_line)
    loop(n_line - 1, lambda step: from_twin(side, by_distance(line, n_line, step, False)))
    loop(n_line - 1, from_across)
    loop(n_line - 1, lambda step: from_twin(1 - side, by_distance(line, n_line, step, False)))
    pl.semaphore_signal(ready, inc=1, device_id=(mirror, me), device_id_type=MESH)

    square = (row_count, row_count)
    down = lax.broadcasted_iota(jnp.int32, square, 0)
    over = lax.broadcasted_iota(jnp.int32, square, 1)
    pairs = jnp.sum(
        jnp.where(down == over, pair_ref[...].astype(jnp.float32), 0.0), axis=1, keepdims=True
    ).astype(jnp.int32)

    def matched(block):
        return over + block * row_count == pairs

    peak = fold(n_dp, lambda p, acc: jnp.maximum(acc, scores[p]), jnp.full(square, -jnp.inf, jnp.float32))
    peak = jnp.max(peak, axis=1, keepdims=True)

    def gather_sums(p, acc):
        total, diagonal = acc
        block = scores[p]
        return total + jnp.exp(block - peak), diagonal + jnp.where(matched(p), block, 0.0)

    zero = jnp.zeros(square, jnp.float32)
    total, diagonal = fold(n_dp, gather_sums, (zero, zero))
    lse = peak + jnp.log(jnp.sum(total, axis=1, keepdims=True))
    excess = lse - jnp.sum(diagonal, axis=1, keepdims=True)

    lanes = note.shape[-1]
    wide = (row_count, lanes)
    lane = lax.broadcasted_iota(jnp.int32, wide, 1)
    placed = jnp.where(
        lane == lax.broadcasted_iota(jnp.int32, wide, 0), lse, jnp.where(lane == lanes - 1, excess, 0.0)
    )
    note[...] = jnp.sum(placed, axis=0, keepdims=True)
    notes[here] = note[...]

    def mirror_target(step):
        if n_line > 8:
            return (me + step) % n_dp
        q = by_distance(line, n_line, step // 4, True) if step // 4 < n_line - 1 else line
        return q * 4 + step % 4

    def note_copy(target_module, target, slot, step):
        return pltpu.make_async_remote_copy(
            src_ref=note, dst_ref=notes.at[slot],
            send_sem=note_send.at[step], recv_sem=note_recv.at[slot],
            device_id=(target_module, target), device_id_type=MESH,
        )

    def mirror_note(step):
        return note_copy(mirror, mirror_target(step), here, step)

    def same_note(step):
        return note_copy(module, (me + 1 + step) % n_dp, here, n_dp + step)

    pl.semaphore_wait(ready, 1)
    loop(n_dp, lambda step: mirror_note(step).start())
    loop(n_dp - 1, lambda step: same_note(step).start())

    def first_half(p):
        base[p] = jnp.exp(scores[p] - lse) - jnp.where(matched(p), 2.0, 0.0)

    loop(n_dp, first_half)

    loop(n_dp, lambda step: note_copy(mirror, step, mirror * n_dp + step, step).wait_recv())

    def weigh(p, acc):
        other = notes[mirror * n_dp + p][:, :row_count]
        weight = (base[p] + jnp.exp(scores[p] - other)).astype(jnp.bfloat16)
        return tuple(
            acc[h] + jnp.dot(weight, rows_all[p, h], preferred_element_type=jnp.float32)
            for h in range(CHUNKS)
        )

    zeros = tuple(jnp.zeros((row_count, depth), jnp.float32) for _ in range(CHUNKS))
    moved = scale_value * jnp.concatenate(fold(n_dp, weigh, zeros), axis=1)
    own = unit[...]
    grad_ref[0] = (moved - own * jnp.sum(own * moved, axis=-1, keepdims=True)) / length[...]

    def same_arrive(step):
        other = (me + 1 + step) % n_dp
        note_copy(module, other, module * n_dp + other, n_dp + step).wait_recv()

    loop(n_dp - 1, same_arrive)
    loss = fold(n_all, lambda p, acc: acc + notes[p], jnp.zeros((1, lanes), jnp.float32))
    loss_ref[...] = loss[:, lanes - 1 :]

    for h in range(CHUNKS):
        loop(n_line - 1, lambda step: line_send(step, h).wait_send())
        loop(n_line, lambda step: across_send(line, h, step).wait_send())
        loop(2 * n_line, lambda step: twin_send(line, side, h, step).wait_send())
    loop(n_dp, lambda step: mirror_note(step).wait_send())
    loop(n_dp - 1, lambda step: same_note(step).wait_send())


def solution(mesh):
    n_mod, n_dp = mesh.shape["mod"], mesh.shape["dp"]

    def local(
        image_pooled, text_pooled, image_gain, text_gain, image_proj, text_proj, logit_scale, pair_index
    ):
        rows = image_pooled.shape[0]
        width = image_proj.shape[1]
        lanes = -(-(rows + 1) // 128) * 128
        n_all = n_mod * n_dp
        vmem = pl.BlockSpec(memory_space=pltpu.VMEM)
        dma = pltpu.SemaphoreType.DMA
        loss, grad = pl.pallas_call(
            functools.partial(kernel, n_mod, n_dp),
            out_shape=(
                jax.ShapeDtypeStruct((1, 1), jnp.float32),
                jax.ShapeDtypeStruct((1, rows, width), jnp.float32),
            ),
            in_specs=[pl.BlockSpec(memory_space=pltpu.HBM)] * 8,
            out_specs=(vmem, vmem),
            scratch_shapes=[
                pltpu.VMEM(image_pooled.shape, image_pooled.dtype),
                pltpu.VMEM(text_pooled.shape, text_pooled.dtype),
                pltpu.VMEM(image_gain.shape, jnp.float32),
                pltpu.VMEM(text_gain.shape, jnp.float32),
                pltpu.SMEM((1,), jnp.float32),
                pltpu.VMEM(pair_index.shape, pair_index.dtype),
                pltpu.VMEM(image_proj.shape, image_proj.dtype),
                pltpu.VMEM(text_proj.shape, text_proj.dtype),
                pltpu.VMEM((n_dp, CHUNKS, rows, width // CHUNKS), jnp.bfloat16),
                pltpu.VMEM((rows, width), jnp.float32),
                pltpu.VMEM((rows, 1), jnp.float32),
                pltpu.VMEM((n_dp, rows, rows), jnp.float32),
                pltpu.VMEM((n_dp, rows, rows), jnp.float32),
                pltpu.VMEM((1, lanes), jnp.float32),
                pltpu.VMEM((n_all, 1, lanes), jnp.float32),
                dma((6,)),
                dma((2,)),
                dma((n_dp, CHUNKS)),
                dma((n_dp, CHUNKS)),
                dma((n_all,)),
                dma((n_all,)),
                pltpu.SemaphoreType.REGULAR,
            ],
            compiler_params=pltpu.CompilerParams(collective_id=0, has_side_effects=True),
        )(image_pooled, text_pooled, image_gain, text_gain, image_proj, text_proj, logit_scale, pair_index)
        batch_total = 2.0 * n_dp * rows
        return loss[0, 0] / batch_total, grad / batch_total

    in_specs = (P("dp", None), P("dp", None), P(), P(), P(), P(), P(), P("mod", "dp"))
    out_specs = (P(), P("mod", "dp", None))
    return jax.shard_map(local, mesh=mesh, in_specs=in_specs, out_specs=out_specs, check_vma=False)
```

```python
import functools

import jax
import jax.numpy as jnp
from jax import lax
from jax.experimental import pallas as pl
from jax.experimental.pallas import tpu as pltpu
from jax.sharding import PartitionSpec as P

MESH = pl.DeviceIdType.MESH
UNROLL = 32
CHUNKS = 2
SLICES = 1


def pick(index, values):
    chosen = 0
    for at, value in enumerate(values):
        chosen = chosen + jnp.where(index == at, value, 0)
    return chosen


def by_distance(index, count, step, far):
    if count > 8:
        return (index + 1 + step) % count
    tables = [
        sorted((p for p in range(count) if p != i), key=lambda p: -abs(p - i) if far else abs(p - i))[step]
        for i in range(count)
    ]
    return pick(index, tables)


def loop(count, body):
    if count <= UNROLL:
        for step in range(count):
            body(step)
    else:
        pl.loop(0, count)(body)


def fold(count, body, init):
    if count <= UNROLL:
        for step in range(count):
            init = body(step, init)
        return init
    return lax.fori_loop(0, count, body, init)


def kernel(
    n_mod, n_dp,
    image_hbm, text_hbm, image_gain_hbm, text_gain_hbm, image_proj_ref, text_proj_ref, scale_ref, pair_hbm,
    loss_ref, grad_ref,
    image_ref, text_ref, image_gain_ref, text_gain_ref, pair_ref,
    image_w, text_w, rows_all, unit, length, scores, base, note, notes,
    in_sem, w_sem, send_sem, recv_sem, note_send, note_recv, ready,
):
    module, me = lax.axis_index("mod"), lax.axis_index("dp")
    n_all = n_mod * n_dp
    n_line = n_dp // 4
    line, side, core = me // 4, (me // 2) % 2, me % 2
    here = module * n_dp + me
    row_count = image_ref.shape[0]
    across = (line * 2 + (1 - side)) * 2 + core
    twin = me + 1 - 2 * core
    mirror = 1 - module

    def peer(q, b, c):
        return (q * 2 + b) * 2 + c

    barrier = pltpu.get_barrier_semaphore()

    def greet(target_module, target):
        pl.semaphore_signal(barrier, inc=1, device_id=(target_module, target), device_id_type=MESH)

    loop(n_line - 1, lambda step: greet(module, peer((line + step + 1) % n_line, side, core)))
    greet(module, across)
    greet(module, twin)
    greet(mirror, me)

    def slices(source, target, at):
        tall = source.shape[0] // SLICES
        return [
            pltpu.make_async_copy(
                source.at[pl.ds(k * tall, tall)], target.at[pl.ds(k * tall, tall)], w_sem.at[at, k]
            )
            for k in range(SLICES)
        ]

    image_copy, text_copy = slices(image_proj_ref, image_w, 0), slices(text_proj_ref, text_w, 1)

    def start(copies):
        for copy in copies:
            copy.start()

    small = [
        pltpu.make_async_copy(source, target, in_sem.at[at])
        for at, (source, target) in enumerate([
            (image_hbm, image_ref), (text_hbm, text_ref), (image_gain_hbm, image_gain_ref),
            (text_gain_hbm, text_gain_ref), (pair_hbm, pair_ref),
        ])
    ]
    for copy in small[:4]:
        copy.start()

    @pl.when(module == 0)
    def _():
        start(text_copy)
        start(image_copy)

    @pl.when(module != 0)
    def _():
        start(image_copy)
        start(text_copy)

    for copy in small[4:]:
        copy.start()
    for copy in small:
        copy.wait()

    def embed(pooled_ref, gain_ref, copies, w):
        features = pooled_ref[...].astype(jnp.float32)
        centered = features - jnp.mean(features, axis=-1, keepdims=True)
        variance = jnp.mean(centered * centered, axis=-1, keepdims=True)
        normed = centered * lax.rsqrt(variance + 1e-05) * gain_ref[...].reshape(1, -1)
        normed = normed.astype(jnp.bfloat16)
        tall = w.shape[0] // SLICES
        embedded = 0.0
        for k in range(SLICES):
            copies[k].wait()
            embedded = embedded + jnp.dot(
                normed[:, k * tall : (k + 1) * tall], w[k * tall : (k + 1) * tall],
                preferred_element_type=jnp.float32,
            )
        lengths = jnp.sqrt(jnp.sum(embedded * embedded, axis=-1, keepdims=True) + 1e-06)
        return embedded / lengths, lengths

    depth = rows_all.shape[-1]

    def embed_other(*args):
        rows = embed(*args)[0].astype(jnp.bfloat16)
        for h in range(CHUNKS):
            rows_all[me, h] = rows[:, h * depth : (h + 1) * depth]

    def embed_own(*args):
        unit[...], length[...] = embed(*args)

    image_args = (image_ref, image_gain_ref, image_copy, image_w)
    text_args = (text_ref, text_gain_ref, text_copy, text_w)

    pl.when(module == 0)(lambda: embed_other(*text_args))
    pl.when(module != 0)(lambda: embed_other(*image_args))

    pl.semaphore_wait(barrier, n_line + 2)

    def send(block, h, target, sem):
        return pltpu.make_async_remote_copy(
            src_ref=rows_all.at[block, h], dst_ref=rows_all.at[block, h],
            send_sem=send_sem.at[sem, h], recv_sem=recv_sem.at[block, h],
            device_id=(module, target), device_id_type=MESH,
        )

    def line_send(step, h):
        return send(me, h, peer(by_distance(line, n_line, step, True), side, core), step)

    def across_send(q, h, step):
        return send(peer(q, side, core), h, across, n_line + step)

    def twin_send(q, b, h, step):
        return send(peer(q, b, core), h, twin, n_line * 2 + step)

    for h in range(CHUNKS):
        across_send(line, h, 0).start()
        loop(n_line - 1, lambda step: line_send(step, h).start())
        twin_send(line, side, h, 0).start()

    pl.when(module == 0)(lambda: embed_own(*image_args))
    pl.when(module != 0)(lambda: embed_own(*text_args))
    own_half = unit[...].astype(jnp.bfloat16)
    scale_value = scale_ref[...].reshape(1, 1)

    def score(block):
        products = 0.0
        for h in range(CHUNKS):
            products = products + lax.dot_general(
                own_half[:, h * depth : (h + 1) * depth], rows_all[block, h],
                (((1,), (1,)), ((), ())), preferred_element_type=jnp.float32,
            )
        scores[block] = scale_value * products

    def arrive(block, h):
        send(block, h, twin, 0).wait_recv()

    score(me)

    for h in range(CHUNKS):
        arrive(across, h)
        twin_send(line, 1 - side, h, n_line).start()
    score(across)

    def from_line(step):
        q = by_distance(line, n_line, step, False)
        for h in range(CHUNKS):
            arrive(peer(q, side, core), h)
            across_send(q, h, step + 1).start()
            twin_send(q, side, h, step + 1).start()
        score(peer(q, side, core))

    def from_across(step):
        q = by_distance(line, n_line, step, False)
        for h in range(CHUNKS):
            arrive(peer(q, 1 - side, core), h)
            twin_send(q, 1 - side, h, n_line + step + 1).start()
        score(peer(q, 1 - side, core))

    def from_twin(b, q):
        block = peer(q, b, 1 - core)
        for h in range(CHUNKS):
            arrive(block, h)
        score(block)

    from_twin(side, line)
    from_twin(1 - side, line)
    loop(n_line - 1, from_line)
    loop(n_line - 1, lambda step: from_twin(side, by_distance(line, n_line, step, False)))
    loop(n_line - 1, from_across)
    loop(n_line - 1, lambda step: from_twin(1 - side, by_distance(line, n_line, step, False)))
    pl.semaphore_signal(ready, inc=1, device_id=(mirror, me), device_id_type=MESH)

    square = (row_count, row_count)
    down = lax.broadcasted_iota(jnp.int32, square, 0)
    over = lax.broadcasted_iota(jnp.int32, square, 1)
    pairs = jnp.sum(
        jnp.where(down == over, pair_ref[...].astype(jnp.float32), 0.0), axis=1, keepdims=True
    ).astype(jnp.int32)

    def matched(block):
        return over + block * row_count == pairs

    peak = fold(n_dp, lambda p, acc: jnp.maximum(acc, scores[p]), jnp.full(square, -jnp.inf, jnp.float32))
    peak = jnp.max(peak, axis=1, keepdims=True)

    def gather_sums(p, acc):
        total, diagonal = acc
        block = scores[p]
        return total + jnp.exp(block - peak), diagonal + jnp.where(matched(p), block, 0.0)

    zero = jnp.zeros(square, jnp.float32)
    total, diagonal = fold(n_dp, gather_sums, (zero, zero))
    lse = peak + jnp.log(jnp.sum(total, axis=1, keepdims=True))
    excess = lse - jnp.sum(diagonal, axis=1, keepdims=True)

    lanes = note.shape[-1]
    wide = (row_count, lanes)
    lane = lax.broadcasted_iota(jnp.int32, wide, 1)
    placed = jnp.where(
        lane == lax.broadcasted_iota(jnp.int32, wide, 0), lse, jnp.where(lane == lanes - 1, excess, 0.0)
    )
    note[...] = jnp.sum(placed, axis=0, keepdims=True)
    notes[here] = note[...]

    def mirror_target(step):
        if n_line > 8:
            return (me + step) % n_dp
        q = by_distance(line, n_line, step // 4, True) if step // 4 < n_line - 1 else line
        return q * 4 + step % 4

    def note_copy(target_module, target, slot, step):
        return pltpu.make_async_remote_copy(
            src_ref=note, dst_ref=notes.at[slot],
            send_sem=note_send.at[step], recv_sem=note_recv.at[slot],
            device_id=(target_module, target), device_id_type=MESH,
        )

    def mirror_note(step):
        return note_copy(mirror, mirror_target(step), here, step)

    def same_note(step):
        return note_copy(module, (me + 1 + step) % n_dp, here, n_dp + step)

    pl.semaphore_wait(ready, 1)
    loop(n_dp, lambda step: mirror_note(step).start())
    loop(n_dp - 1, lambda step: same_note(step).start())

    def first_half(p):
        base[p] = jnp.exp(scores[p] - lse) - jnp.where(matched(p), 2.0, 0.0)

    loop(n_dp, first_half)

    loop(n_dp, lambda step: note_copy(mirror, step, mirror * n_dp + step, step).wait_recv())

    def weigh(p, acc):
        other = notes[mirror * n_dp + p][:, :row_count]
        weight = (base[p] + jnp.exp(scores[p] - other)).astype(jnp.bfloat16)
        return tuple(
            acc[h] + jnp.dot(weight, rows_all[p, h], preferred_element_type=jnp.float32)
            for h in range(CHUNKS)
        )

    zeros = tuple(jnp.zeros((row_count, depth), jnp.float32) for _ in range(CHUNKS))
    moved = scale_value * jnp.concatenate(fold(n_dp, weigh, zeros), axis=1)
    own = unit[...]
    grad_ref[0] = (moved - own * jnp.sum(own * moved, axis=-1, keepdims=True)) / length[...]

    def same_arrive(step):
        other = (me + 1 + step) % n_dp
        note_copy(module, other, module * n_dp + other, n_dp + step).wait_recv()

    loop(n_dp - 1, same_arrive)
    loss = fold(n_all, lambda p, acc: acc + notes[p], jnp.zeros((1, lanes), jnp.float32))
    loss_ref[...] = loss[:, lanes - 1 :]

    for h in range(CHUNKS):
        loop(n_line - 1, lambda step: line_send(step, h).wait_send())
        loop(n_line, lambda step: across_send(line, h, step).wait_send())
        loop(2 * n_line, lambda step: twin_send(line, side, h, step).wait_send())
    loop(n_dp, lambda step: mirror_note(step).wait_send())
    loop(n_dp - 1, lambda step: same_note(step).wait_send())


def solution(mesh):
    n_mod, n_dp = mesh.shape["mod"], mesh.shape["dp"]

    def local(
        image_pooled, text_pooled, image_gain, text_gain, image_proj, text_proj, logit_scale, pair_index
    ):
        rows = image_pooled.shape[0]
        width = image_proj.shape[1]
        lanes = -(-(rows + 1) // 128) * 128
        n_all = n_mod * n_dp
        vmem = pl.BlockSpec(memory_space=pltpu.VMEM)
        dma = pltpu.SemaphoreType.DMA
        loss, grad = pl.pallas_call(
            functools.partial(kernel, n_mod, n_dp),
            out_shape=(
                pltpu.VMEM((1, 1), jnp.float32),
                pltpu.VMEM((1, rows, width), jnp.float32),
            ),
            in_specs=[pl.BlockSpec(memory_space=pltpu.HBM)] * 6
            + [vmem, pl.BlockSpec(memory_space=pltpu.HBM)],
            out_specs=(vmem, vmem),
            scratch_shapes=[
                pltpu.VMEM(image_pooled.shape, image_pooled.dtype),
                pltpu.VMEM(text_pooled.shape, text_pooled.dtype),
                pltpu.VMEM(image_gain.shape, jnp.float32),
                pltpu.VMEM(text_gain.shape, jnp.float32),
                pltpu.VMEM(pair_index.shape, pair_index.dtype),
                pltpu.VMEM(image_proj.shape, image_proj.dtype),
                pltpu.VMEM(text_proj.shape, text_proj.dtype),
                pltpu.VMEM((n_dp, CHUNKS, rows, width // CHUNKS), jnp.bfloat16),
                pltpu.VMEM((rows, width), jnp.float32),
                pltpu.VMEM((rows, 1), jnp.float32),
                pltpu.VMEM((n_dp, rows, rows), jnp.float32),
                pltpu.VMEM((n_dp, rows, rows), jnp.float32),
                pltpu.VMEM((1, lanes), jnp.float32),
                pltpu.VMEM((n_all, 1, lanes), jnp.float32),
                dma((5,)),
                dma((2, SLICES)),
                dma((n_dp, CHUNKS)),
                dma((n_dp, CHUNKS)),
                dma((n_all,)),
                dma((n_all,)),
                pltpu.SemaphoreType.REGULAR,
            ],
            compiler_params=pltpu.CompilerParams(collective_id=0, has_side_effects=True),
        )(image_pooled, text_pooled, image_gain, text_gain, image_proj, text_proj, logit_scale, pair_index)
        batch_total = 2.0 * n_dp * rows
        return loss[0, 0] / batch_total, grad / batch_total

    in_specs = (P("dp", None), P("dp", None), P(), P(), P(), P(), P(), P("mod", "dp"))
    out_specs = (P(), P("mod", "dp", None))
    return jax.shard_map(local, mesh=mesh, in_specs=in_specs, out_specs=out_specs, check_vma=False)
```
